32 devices in a mesh: seq: 8 (over y, x, core), fsdp: 4 (over z).
Axes of the slice: x: 2, y: 2, z: 4, core: 2. Of those that a mesh axis runs over, the one named last changes fastest.
Arguments:
- hidden: bfloat16 [4096, 8192], P(('seq', 'fsdp')), may hold values from -6 to 6
- kv_blocks: bfloat16 [8192, 1024], P('fsdp'), may hold values from -0.0625 to 0.0625
- kv_scale: float32 [64, 8], P('fsdp'), may hold values from 0.5 to 2
- queries: bfloat16 [4096, 4096], P(('seq', 'fsdp')), may hold values from -24 to 24
- grad_out: bfloat16 [4096, 4096], P(('seq', 'fsdp')), may hold values from -6 to 6
Outputs:
- attn_out: bfloat16 [4096, 4096], P(('seq', 'fsdp'))
- grad_queries: bfloat16 [4096, 4096], P(('seq', 'fsdp'))
- grad_hidden: bfloat16 [4096, 8192], P(('seq', 'fsdp'))
- weight_grad: float32 [8192, 1024], P('fsdp')
The draws below stay inside these ranges and needn't reach their ends.
All inputs are finite; a program needn't handle non-finite values.
Results may differ from the reference program's by a relative error of at most 0.0075.
The reference program's roundings to bfloat16 on the way (of `weights`, `kv`, `probs_b` and `dscores`) count: a program that leaves them out, or rounds other values in their place, can miss the bound.
Values may be sent and summed in bfloat16 or wider, within the bound.
A program may use at most 128 MiB of HBM per device.

```python
import math
import jax
import jax.numpy as jnp
from jax import lax

D = 8192
HEADS = 32
KV_HEADS = 4
HEAD = 128
QB = 128
TOK_DEV = 128
KVW = 512
SEG = 512
SPAN = 256
TOKENS = 4096


def draw_queries(key, part):
    shape = (TOKENS, HEADS * HEAD)
    first = jax.random.fold_in(jax.random.fold_in(key, 17), 0)
    return jnp.clip(jax.random.normal(first, shape, jnp.float32), -4.0, 4.0).astype(jnp.bfloat16)


def strengthened(array, rng, source, target, blocks, factor):
    def block_of(axis_at):
        return (jnp.arange(array.shape[axis_at]) // (array.shape[axis_at] // blocks)).reshape((-1,) + (1,) * (array.ndim - 1 - axis_at))

    first = jax.random.permutation(rng, blocks)[block_of(target)]
    far = (block_of(target) + blocks // 2) % blocks
    return jnp.where((block_of(source) == first) | (block_of(source) == far), factor * array, array)


def shard_levels(own_key, shape, cuts, low, top_value):
    gain, own = 1.0, jax.random.fold_in(own_key, 6)
    for axis_at, shards_of in cuts:
        draws = jnp.exp(jax.random.uniform(jax.random.fold_in(own, axis_at), (shards_of,), jnp.float32, low / len(cuts), top_value / len(cuts)))
        gain = gain * jnp.repeat(draws, shape[axis_at] // shards_of).reshape([-1 if axis == axis_at else 1 for axis in range(len(shape))])
    return gain


def centred(key, shape, scale, bound, shards=(), held_as=jnp.bfloat16):
    entries = jax.random.normal(key, shape, jnp.float32) * scale
    if len(shards) > 0:
        entries = shard_levels(key, shape, shards, -0.22, 0.18) * entries
    return jnp.clip(entries, min=-bound, max=bound).astype(held_as)


def noise_with(rng, shape, scale, bound, cuts, heavy, kind=jnp.bfloat16):
    entries = scale * jax.random.normal(rng, shape, jnp.float32)
    if cuts:
        entries = entries * shard_levels(rng, shape, cuts, -0.22, 0.18)
    return jnp.clip(strengthened(entries, jax.random.fold_in(rng, 3), *heavy), -bound, bound).astype(kind)


def setup_inputs(seed: int = 0) -> dict:
    key_list = jax.random.split(jax.random.key(seed), 6)
    return {
        "hidden": noise_with(key_list[0], (TOKENS, D), 1.0, 6.0, ((0, 32),), (0, 1, 32, 2.75)),
        "kv_blocks": centred(key_list[1], (D, 2 * KVW), D ** -0.5, 0.0625, ((0, 4),)),
        "kv_scale": jnp.clip(jnp.exp(math.log(2.0) - 1.3862944 * jax.random.uniform(key_list[2], (D // QB, 2 * KVW // QB), jnp.float32) ** shard_levels(key_list[2], (D // QB, 2 * KVW // QB), ((0, 4),), -0.2, 0.2)), 0.5, 2.0),
        "queries": draw_queries(jax.random.fold_in(key_list[5], 71), 0),
        "grad_out": centred(key_list[4], (TOKENS, HEADS * HEAD), 1.0, 6.0, ((0, 32),)),
    }


NEG = -1e+30

def dequantize(blocks, scale):
    rows, cols = blocks.shape
    grid = blocks.astype(jnp.float32).reshape(scale.shape[0], QB, scale.shape[1], QB)
    return (grid * scale[:, None, :, None]).reshape(rows, cols).astype(jnp.bfloat16)

def attend_group(operands, allowed):
    qgrp, kgrp, vgrp, ggrp = operands
    factor = 1.0 / math_sqrt(HEAD)
    qf = qgrp.astype(jnp.float32)
    kf = kgrp.astype(jnp.float32)
    vf = vgrp.astype(jnp.float32)
    gf = ggrp.astype(jnp.float32)
    scores = jnp.einsum('rhd,kd->rhk', qf, kf) * factor
    scores = jnp.where(allowed[:, None, :], scores, NEG)
    top = lax.optimization_barrier(jnp.max(scores, axis=-1, keepdims=True))
    expd = jnp.exp(scores - top)
    probs = expd / lax.optimization_barrier(jnp.sum(expd, axis=-1, keepdims=True))
    probs_b = probs.astype(jnp.bfloat16)
    pf = probs_b.astype(jnp.float32)
    output = jnp.einsum('rhk,kd->rhd', pf, vf).astype(jnp.bfloat16)
    dprobs = jnp.einsum('rhd,kd->rhk', gf, vf)
    delta = lax.optimization_barrier(jnp.sum(probs * dprobs, axis=-1, keepdims=True))
    dscores = (probs * (dprobs - delta) * factor).astype(jnp.bfloat16)
    df = dscores.astype(jnp.float32)
    gradq = jnp.einsum('rhk,kd->rhd', df, kf).astype(jnp.bfloat16)
    gradk = jnp.einsum('rhk,rhd->kd', df, qf)
    gradv = jnp.einsum('rhk,rhd->kd', pf, gf)
    return (output, gradq, gradk, gradv)

def math_sqrt(value):
    return float(value) ** 0.5

def attend(queries, window, grad_out, allowed):
    rows = queries.shape[0]
    count = window.shape[0]
    group = HEADS // KV_HEADS
    qgrp = queries.reshape(rows, KV_HEADS, group, HEAD).transpose(1, 0, 2, 3)
    ggrp = grad_out.reshape(rows, KV_HEADS, group, HEAD).transpose(1, 0, 2, 3)
    kgrp = window[:, :KVW].reshape(count, KV_HEADS, HEAD).transpose(1, 0, 2)
    vgrp = window[:, KVW:].reshape(count, KV_HEADS, HEAD).transpose(1, 0, 2)
    output, gradq, gradk, gradv = lax.map(lambda ops: attend_group(ops, allowed), (qgrp, kgrp, vgrp, ggrp))
    output = output.transpose(1, 0, 2, 3).reshape(rows, HEADS * HEAD)
    gradq = gradq.transpose(1, 0, 2, 3).reshape(rows, HEADS * HEAD)
    gradk = gradk.transpose(1, 0, 2).reshape(count, KVW)
    gradv = gradv.transpose(1, 0, 2).reshape(count, KVW)
    return (output, gradq, jnp.concatenate([gradk, gradv], axis=1))

def reference(hidden, kv_blocks, kv_scale, queries, grad_out):
    weights = dequantize(kv_blocks, kv_scale)
    kv = jnp.dot(hidden, weights, preferred_element_type=jnp.float32).astype(jnp.bfloat16)
    padded = jnp.concatenate([jnp.zeros((SPAN, 2 * KVW), jnp.bfloat16), kv], axis=0)
    width = SPAN + TOK_DEV
    blocks = TOKENS // TOK_DEV

    def step(carry, index):
        acc_all, acc_seg = carry
        start = (index * TOK_DEV).astype(jnp.int32)
        qrows = lax.dynamic_slice_in_dim(queries, start, TOK_DEV, 0)
        grows = lax.dynamic_slice_in_dim(grad_out, start, TOK_DEV, 0)
        window = lax.dynamic_slice_in_dim(padded, start, width, 0)
        qpos = start + jnp.arange(TOK_DEV, dtype=jnp.int32)
        kpos = start - SPAN + jnp.arange(width, dtype=jnp.int32)
        allowed = (qpos[:, None] - kpos[None, :] < SPAN) & (kpos[None, :] <= qpos[:, None]) & (kpos[None, :] >= 0)
        seg_start = start // SEG * SEG
        inside = (kpos >= seg_start).astype(jnp.float32)
        output, gradq, dwin = attend(qrows, window, grows, allowed)
        old_all = lax.dynamic_slice_in_dim(acc_all, start, width, 0)
        acc_all = lax.dynamic_update_slice_in_dim(acc_all, old_all + dwin, start, 0)
        old_seg = lax.dynamic_slice_in_dim(acc_seg, start, width, 0)
        acc_seg = lax.dynamic_update_slice_in_dim(acc_seg, old_seg + dwin * inside[:, None], start, 0)
        return ((acc_all, acc_seg), (output, gradq))
    zeros = jnp.zeros((SPAN + TOKENS, 2 * KVW), jnp.float32)
    (acc_all, acc_seg), (outputs, gradqs) = lax.scan(step, (zeros, zeros), jnp.arange(blocks, dtype=jnp.int32))
    attn_out = outputs.reshape(TOKENS, HEADS * HEAD)
    grad_queries = gradqs.reshape(TOKENS, HEADS * HEAD)
    dkv_all = acc_all[SPAN:].astype(jnp.bfloat16)
    dkv_seg = acc_seg[SPAN:].astype(jnp.bfloat16)
    grad_hidden = jnp.dot(dkv_seg, weights.T, preferred_element_type=jnp.float32).astype(jnp.bfloat16)
    weight_grad = jnp.dot(hidden.T, dkv_all, preferred_element_type=jnp.float32)
    return (attn_out, grad_queries, grad_hidden, weight_grad)
```

```python
import functools

import jax
import jax.numpy as jnp
from jax import lax
from jax.experimental import pallas as pl
from jax.experimental.pallas import tpu as pltpu
from jax.sharding import PartitionSpec as P

HEADS = 32
KV_HEADS = 4
HEAD = 128
QB = 128


NEG = -1e30


def shifted(block, axis, distance):
    devices = range(lax.axis_size(axis))
    route = [(i - distance, i) for i in devices if i - distance in devices]
    return lax.ppermute(block, axis, route)


def dequantize(blocks, scale):
    rows, cols = blocks.shape
    grid = blocks.astype(jnp.float32).reshape(scale.shape[0], QB, scale.shape[1], QB)
    return (grid * scale[:, None, :, None]).reshape(rows, cols).astype(jnp.bfloat16)


def attend_kernel(reach, q_ref, g_ref, k_ref, v_ref, out_ref, dq_ref, dk_ref, dv_ref):
    tok = q_ref.shape[0]
    group = q_ref.shape[1] // HEAD
    count = k_ref.shape[0]
    span = reach * tok
    factor = 1.0 / float(HEAD) ** 0.5
    base = (lax.axis_index("seq") * lax.axis_size("fsdp") + lax.axis_index("fsdp")) * tok
    row = lax.broadcasted_iota(jnp.int32, (tok, count), 0)
    col = lax.broadcasted_iota(jnp.int32, (tok, count), 1)
    allowed = (col > row) & (col <= row + span) & (col >= span - base)
    keys = k_ref[...]
    values = v_ref[...]
    nt = (((1,), (1,)), ((), ()))
    tn = (((0,), (0,)), ((), ()))
    ps, ds, qs, gs = [], [], [], []
    for h in range(group):
        cut = slice(h * HEAD, (h + 1) * HEAD)
        q = q_ref[:, cut]
        g = g_ref[:, cut]
        scores = lax.dot_general(q, keys, nt, preferred_element_type=jnp.float32) * factor
        scores = jnp.where(allowed, scores, NEG)
        expd = jnp.exp(scores - jnp.max(scores, axis=-1, keepdims=True))
        probs = expd * (1.0 / jnp.sum(expd, axis=-1, keepdims=True))
        probs_b = probs.astype(jnp.bfloat16)
        out_ref[:, cut] = jnp.dot(probs_b, values, preferred_element_type=jnp.float32).astype(jnp.bfloat16)
        dprobs = lax.dot_general(g, values, nt, preferred_element_type=jnp.float32)
        delta = jnp.sum(probs * dprobs, axis=-1, keepdims=True)
        dscores = (probs * (dprobs - delta) * factor).astype(jnp.bfloat16)
        dq_ref[:, cut] = jnp.dot(dscores, keys, preferred_element_type=jnp.float32).astype(jnp.bfloat16)
        ps.append(probs_b)
        ds.append(dscores)
        qs.append(q)
        gs.append(g)
    cat = lambda parts: jnp.concatenate(parts, axis=0)
    dk_ref[...] = lax.dot_general(cat(ds), cat(qs), tn, preferred_element_type=jnp.float32)
    dv_ref[...] = lax.dot_general(cat(ps), cat(gs), tn, preferred_element_type=jnp.float32)


def attend(queries, window, grad_out, reach):
    tok, width = queries.shape
    count = window.shape[0]
    heads = window.shape[1] // (2 * HEAD)
    wide = pl.BlockSpec((tok, width // heads), lambda i: (0, i))
    key = pl.BlockSpec((count, HEAD), lambda i: (0, i))
    value = pl.BlockSpec((count, HEAD), lambda i: (0, i + heads))
    out, dq, dk, dv = pl.pallas_call(
        functools.partial(attend_kernel, reach),
        grid=(heads,),
        in_specs=[wide, wide, key, value],
        out_specs=[wide, wide, key, key],
        out_shape=[
            jax.ShapeDtypeStruct((tok, width), jnp.bfloat16),
            jax.ShapeDtypeStruct((tok, width), jnp.bfloat16),
            jax.ShapeDtypeStruct((count, heads * HEAD), jnp.float32),
            jax.ShapeDtypeStruct((count, heads * HEAD), jnp.float32),
        ],
        cost_estimate=pl.CostEstimate(flops=12 * tok * width * count, bytes_accessed=8 * tok * width, transcendentals=0),
        name="attend",
    )(queries, grad_out, window, window)
    return out, dq, jnp.concatenate([dk, dv], axis=1)


def body(hidden, kv_blocks, kv_scale, queries, grad_out):
    tok = hidden.shape[0]
    groups = lax.axis_size("fsdp")
    reach = groups // 2
    place = lax.axis_index("fsdp")
    linear = lax.axis_index("seq") * groups + place
    weights = dequantize(kv_blocks, kv_scale)
    columns = lax.all_to_all(hidden, "fsdp", split_axis=1, concat_axis=0, tiled=True)
    rows = columns
    kv = lax.psum_scatter(
        jnp.dot(rows, weights, preferred_element_type=jnp.float32),
        "fsdp",
        scatter_dimension=0,
        tiled=True,
    ).astype(jnp.bfloat16)
    pieces = []
    for offset in range(reach, 0, -1):
        pieces.append(shifted(kv, ("seq", "fsdp"), offset))
    window = jnp.concatenate(pieces + [kv], axis=0)
    attn_out, grad_queries, dwin = attend(queries, window, grad_out, reach)
    total = dwin[reach * tok :]
    inside = total
    for offset in range(1, reach + 1):
        piece = dwin[(reach - offset) * tok : (reach - offset + 1) * tok]
        returned = shifted(piece, ("seq", "fsdp"), -offset)
        total = total + returned
        inside = inside + jnp.where(place + offset < groups, returned, jnp.zeros_like(returned))
    all_grad = total.astype(jnp.bfloat16)
    seg_grad = inside.astype(jnp.bfloat16)
    spread = lax.dot_general(
        lax.all_gather(seg_grad, "fsdp", axis=0, tiled=True),
        weights,
        (((1,), (1,)), ((), ())),
        preferred_element_type=jnp.float32,
    ).astype(jnp.bfloat16)
    grad_hidden = lax.all_to_all(spread, "fsdp", split_axis=0, concat_axis=1, tiled=True)
    rows = columns
    shard_grad = lax.dot_general(
        rows,
        lax.all_gather(all_grad, "fsdp", axis=0, tiled=True),
        (((0,), (0,)), ((), ())),
        preferred_element_type=jnp.float32,
    )
    weight_grad = lax.psum(shard_grad.astype(jnp.bfloat16), "seq").astype(jnp.float32)
    return (attn_out, grad_queries, grad_hidden, weight_grad)


def solution(mesh):
    return jax.shard_map(
        body,
        mesh=mesh,
        in_specs=(
            P(("seq", "fsdp"), None),
            P("fsdp", None),
            P("fsdp", None),
            P(("seq", "fsdp"), None),
            P(("seq", "fsdp"), None),
        ),
        out_specs=(
            P(("seq", "fsdp"), None),
            P(("seq", "fsdp"), None),
            P(("seq", "fsdp"), None),
            P("fsdp", None),
        ),
        check_vma=False,
    )
```

```python
import functools

import jax
import jax.numpy as jnp
from jax import lax
from jax.experimental import pallas as pl
from jax.experimental.pallas import tpu as pltpu
from jax.sharding import PartitionSpec as P

HEADS = 32
KV_HEADS = 4
HEAD = 128
QB = 128


NEG = -1e30


def shifted(block, axis, distance):
    devices = range(lax.axis_size(axis))
    route = [(i - distance, i) for i in devices if i - distance in devices]
    return lax.ppermute(block, axis, route)


def attend_kernel(reach, q_ref, g_ref, k_ref, v_ref, out_ref, dq_ref, dk_ref, dv_ref):
    tok = q_ref.shape[0]
    group = q_ref.shape[1] // HEAD
    count = k_ref.shape[0]
    span = reach * tok
    factor = 1.0 / float(HEAD) ** 0.5
    base = (lax.axis_index("seq") * lax.axis_size("fsdp") + lax.axis_index("fsdp")) * tok
    row = lax.broadcasted_iota(jnp.int32, (tok, count), 0)
    col = lax.broadcasted_iota(jnp.int32, (tok, count), 1)
    allowed = (col > row) & (col <= row + span) & (col >= span - base)
    keys = k_ref[...]
    values = v_ref[...]
    nt = (((1,), (1,)), ((), ()))
    tn = (((0,), (0,)), ((), ()))
    ps, ds, qs, gs = [], [], [], []
    for h in range(group):
        cut = slice(h * HEAD, (h + 1) * HEAD)
        q = q_ref[:, cut]
        g = g_ref[:, cut]
        scores = lax.dot_general(q, keys, nt, preferred_element_type=jnp.float32) * factor
        scores = jnp.where(allowed, scores, NEG)
        expd = jnp.exp(scores - jnp.max(scores, axis=-1, keepdims=True))
        probs = expd * (1.0 / jnp.sum(expd, axis=-1, keepdims=True))
        probs_b = probs.astype(jnp.bfloat16)
        out_ref[:, cut] = jnp.dot(probs_b, values, preferred_element_type=jnp.float32).astype(jnp.bfloat16)
        dprobs = lax.dot_general(g, values, nt, preferred_element_type=jnp.float32)
        delta = jnp.sum(probs * dprobs, axis=-1, keepdims=True)
        dscores = (probs * (dprobs - delta) * factor).astype(jnp.bfloat16)
        dq_ref[:, cut] = jnp.dot(dscores, keys, preferred_element_type=jnp.float32).astype(jnp.bfloat16)
        ps.append(probs_b)
        ds.append(dscores)
        qs.append(q)
        gs.append(g)
    cat = lambda parts: jnp.concatenate(parts, axis=0)
    dk_ref[...] = lax.dot_general(cat(ds), cat(qs), tn, preferred_element_type=jnp.float32)
    dv_ref[...] = lax.dot_general(cat(ps), cat(gs), tn, preferred_element_type=jnp.float32)


def attend(queries, window, grad_out, reach):
    tok, width = queries.shape
    count = window.shape[0]
    heads = window.shape[1] // (2 * HEAD)
    wide = pl.BlockSpec((tok, width // heads), lambda i: (0, i))
    key = pl.BlockSpec((count, HEAD), lambda i: (0, i))
    value = pl.BlockSpec((count, HEAD), lambda i: (0, i + heads))
    out, dq, dk, dv = pl.pallas_call(
        functools.partial(attend_kernel, reach),
        grid=(heads,),
        in_specs=[wide, wide, key, value],
        out_specs=[wide, wide, key, key],
        out_shape=[
            jax.ShapeDtypeStruct((tok, width), jnp.bfloat16),
            jax.ShapeDtypeStruct((tok, width), jnp.bfloat16),
            jax.ShapeDtypeStruct((count, heads * HEAD), jnp.float32),
            jax.ShapeDtypeStruct((count, heads * HEAD), jnp.float32),
        ],
        cost_estimate=pl.CostEstimate(flops=12 * tok * width * count, bytes_accessed=8 * tok * width, transcendentals=0),
        name="attend",
    )(queries, grad_out, window, window)
    return out, dq, jnp.concatenate([dk, dv], axis=1)


def flipped(index, mask):
    for place in range(mask.bit_length()):
        if mask >> place & 1:
            index = index + (1 << place) * (1 - 2 * (index // (1 << place) % 2))
    return index


def orders_of(bits):
    return (list(range(1, bits)) + [0], list(range(bits - 1, 0, -1)) + [0])


def project_kernel(seqs, groups, hid_ref, blk_ref, sc_ref, w_ref, kv_ref, acc, zsend, zrecv, qsend, qrecv):
    s = lax.axis_index("seq")
    z = lax.axis_index("fsdp")
    rows = blk_ref.shape[0]
    unit = rows // seqs
    half = unit // 2
    bits = seqs.bit_length() - 1
    chunk = min(512, rows)

    def scale_block(i, carry):
        at = pl.multiple_of(i * QB, QB)
        block = blk_ref[pl.ds(at, QB), :].astype(jnp.float32) * sc_ref[pl.ds(i, 1), :]
        w_ref[pl.ds(pl.multiple_of(z * rows + at, QB), QB), :] = block.astype(jnp.bfloat16)
        return carry

    lax.fori_loop(0, rows // QB, scale_block, 0)

    def line_copy(shard, up):
        piece = w_ref.at[pl.ds(pl.multiple_of(shard * rows + s * unit, 16), unit), :]
        return pltpu.make_async_remote_copy(
            src_ref=piece,
            dst_ref=piece,
            send_sem=zsend.at[up, shard],
            recv_sem=zrecv.at[shard],
            device_id=(s, z + 1 if up else z - 1),
            device_id_type=pl.DeviceIdType.MESH,
        )

    def cube_copy(turn, shard, order, step, which, incoming):
        bit = order[step]
        mask = 0
        for k in range(step):
            if which >> k & 1:
                mask |= 1 << order[k]
        h = 0 if order is orders[0] else 1
        owner = flipped(s, mask | (1 << bit) if incoming else mask)
        piece = w_ref.at[pl.ds(pl.multiple_of(shard * rows + owner * unit + h * half, 16), half), :]
        slot = (1 << step) - 1 + which
        return pltpu.make_async_remote_copy(
            src_ref=piece,
            dst_ref=piece,
            send_sem=qsend.at[turn, h, slot],
            recv_sem=qrecv.at[turn, h, slot],
            device_id=(flipped(s, 1 << bit), z),
            device_id_type=pl.DeviceIdType.MESH,
        )

    orders = orders_of(bits)
    near = jnp.minimum(z, groups - 1 - z)

    def shard_at(turn):
        step = turn // 2 + 1
        paired = z - step if turn % 2 == 0 else z + step
        far = turn - near + 1
        single = jnp.where(z > groups - 1 - z, z - far, z + far)
        return jnp.where(turn < 2 * near, paired, single)

    shards = [shard_at(turn) for turn in range(groups - 1)]

    @pl.when(z < groups - 1)
    def _():
        line_copy(z, 1).start()

    @pl.when(z > 0)
    def _():
        line_copy(z, 0).start()

    acc[...] = jnp.zeros_like(acc)

    def multiply(shard):
        def part(i, carry):
            at = pl.multiple_of(shard * rows + i * chunk, 128)
            acc[...] += jnp.dot(
                hid_ref[:, pl.ds(at, chunk)], w_ref[pl.ds(at, chunk), :], preferred_element_type=jnp.float32
            )
            return carry

        lax.fori_loop(0, rows // chunk, part, 0)

    multiply(z)
    for tick in range(groups - 1 + bits):
        for stage in range(bits, -1, -1):
            turn = tick - stage
            if turn < 0 or turn >= groups - 1:
                continue
            shard = shards[turn]
            if stage == 0:
                line_copy(shard, 0).wait_recv()

                @pl.when((shard < z) & (z < groups - 1))
                def _():
                    line_copy(shard, 1).start()

                @pl.when((shard > z) & (z > 0))
                def _():
                    line_copy(shard, 0).start()
            else:
                for order in orders:
                    for which in range(1 << (stage - 1)):
                        cube_copy(turn, shard, order, stage - 1, which, True).wait_recv()
            if stage < bits:
                for order in orders:
                    for which in range(1 << stage):
                        cube_copy(turn, shard, order, stage, which, False).start()
            else:
                multiply(shard)
    kv_ref[...] = acc[...].astype(jnp.bfloat16)
    for shard in range(groups):

        @pl.when((shard <= z) & (z < groups - 1))
        def _():
            line_copy(shard, 1).wait_send()

        @pl.when((shard >= z) & (z > 0))
        def _():
            line_copy(shard, 0).wait_send()

    for turn in range(groups - 1):
        for order in orders:
            for stage in range(bits):
                for which in range(1 << stage):
                    cube_copy(turn, shards[turn], order, stage, which, False).wait_send()


def project(hidden, kv_blocks, kv_scale):
    seqs = lax.axis_size("seq")
    groups = lax.axis_size("fsdp")
    tok, width = hidden.shape
    cols = kv_blocks.shape[1]
    spread = jnp.repeat(kv_scale, QB, axis=1)
    vmem = pl.BlockSpec(memory_space=pltpu.VMEM)
    return pl.pallas_call(
        functools.partial(project_kernel, seqs, groups),
        out_shape=[
            jax.ShapeDtypeStruct((width, cols), jnp.bfloat16),
            jax.ShapeDtypeStruct((tok, cols), jnp.bfloat16),
        ],
        in_specs=[vmem] * 3,
        out_specs=[vmem] * 2,
        scratch_shapes=[
            pltpu.VMEM((tok, cols), jnp.float32),
            pltpu.SemaphoreType.DMA((2, groups)),
            pltpu.SemaphoreType.DMA((groups,)),
            pltpu.SemaphoreType.DMA((groups - 1, 2, seqs - 1)),
            pltpu.SemaphoreType.DMA((groups - 1, 2, seqs - 1)),
        ],
        compiler_params=pltpu.CompilerParams(has_side_effects=True),
        name="project",
    )(hidden, kv_blocks, spread)


def finish_kernel(
    seqs, groups, reach, back_ref, own_ref, w_ref, col_ref, gh_ref, wg_ref,
    ret, every, inside, acc, sends, recvs, hsend, hrecv, gsend, grecv, rsend, rrecv, asend, arecv,
):
    s = lax.axis_index("seq")
    z = lax.axis_index("fsdp")
    linear = s * groups + z
    devices = seqs * groups
    tok, cols = own_ref.shape
    rows = col_ref.shape[1]
    bits = seqs.bit_length() - 1
    mesh_id = pl.DeviceIdType.MESH

    def halo_copy(offset, incoming):
        other = linear + offset if incoming else linear - offset
        return pltpu.make_async_remote_copy(
            src_ref=back_ref.at[pl.ds((reach - offset) * tok, tok), :],
            dst_ref=ret.at[offset - 1],
            send_sem=hsend.at[offset - 1],
            recv_sem=hrecv.at[offset - 1],
            device_id=(other // groups, other % groups),
            device_id_type=mesh_id,
        )

    for offset in range(1, reach + 1):

        @pl.when(linear >= offset)
        def _():
            halo_copy(offset, False).start()

    for offset in range(1, reach + 1):

        @pl.when(linear + offset < devices)
        def _():
            halo_copy(offset, True).wait_recv()

        @pl.when(linear + offset >= devices)
        def _():
            ret[offset - 1] = jnp.zeros((tok, cols), jnp.bfloat16)

    total = own_ref[...]
    seg = total
    for offset in range(1, reach + 1):
        piece = ret[offset - 1].astype(jnp.float32)
        total = total + piece
        seg = seg + piece * jnp.where(z + offset < groups, 1.0, 0.0)
    every[z] = total.astype(jnp.bfloat16)
    inside[...] = seg.astype(jnp.bfloat16)

    def gather_copy(gap, incoming):
        other = (z - gap + groups) % groups if incoming else (z + gap) % groups
        block = every.at[other if incoming else z]
        return pltpu.make_async_remote_copy(
            src_ref=block,
            dst_ref=block,
            send_sem=gsend.at[gap - 1],
            recv_sem=grecv.at[gap - 1],
            device_id=(s, other),
            device_id_type=mesh_id,
        )

    for gap in range(1, groups):
        gather_copy(gap, False).start()

    wide = 512

    def spread(i, carry):
        at = pl.multiple_of(i * wide, wide)
        gh_ref[:, pl.ds(at, wide)] = lax.dot_general(
            inside[...], w_ref[pl.ds(at, wide), :], (((1,), (1,)), ((), ())), preferred_element_type=jnp.float32
        ).astype(jnp.bfloat16)
        return carry

    lax.fori_loop(0, w_ref.shape[0] // wide, spread, 0)
    for gap in range(1, groups):
        gather_copy(gap, True).wait_recv()

    big = rows // 2
    tile = min(256, big)
    low = s % 2
    sibling = flipped(s, 1)
    grads = every[...].reshape(groups * tok, cols)

    def product(at):
        return lax.dot_general(
            col_ref[:, pl.ds(at, tile)], grads, (((0,), (0,)), ((), ())), preferred_element_type=jnp.float32
        )

    def theirs(i, carry):
        at = pl.multiple_of(i * tile, tile)
        sends[0][pl.ds(at, tile), :] = product(pl.multiple_of((1 - low) * big + at, tile)).astype(jnp.bfloat16)
        return carry

    lax.fori_loop(0, big // tile, theirs, 0)

    def reduce_copy(step, h, peer):
        cut = slice(None) if h is None else pl.ds(h * (cols // 2), cols // 2)
        return pltpu.make_async_remote_copy(
            src_ref=sends[step].at[:, cut] if h is not None else sends[step],
            dst_ref=recvs[step].at[:, cut] if h is not None else recvs[step],
            send_sem=rsend.at[step, h or 0],
            recv_sem=rrecv.at[step, h or 0],
            device_id=(peer, z),
            device_id_type=mesh_id,
        )

    reduce_copy(0, None, sibling).start()

    def mine(i, carry):
        at = pl.multiple_of(i * tile, tile)
        acc[pl.ds(at, tile), :] = product(pl.multiple_of(low * big + at, tile))
        return carry

    lax.fori_loop(0, big // tile, mine, 0)
    reduce_copy(0, None, sibling).wait_recv()

    def fold(i, carry):
        at = pl.multiple_of(i * tile, tile)
        acc[pl.ds(at, tile), :] += recvs[0][pl.ds(at, tile), :].astype(jnp.float32)
        return carry

    lax.fori_loop(0, big // tile, fold, 0)
    orders = (list(range(1, bits)), list(range(bits - 1, 0, -1)))
    offsets = [[0], [0]]
    side = cols // 2
    for step in range(1, bits):
        size = rows >> (step + 1)
        for h in range(2):
            place = orders[h][step - 1]
            bit = s // (1 << place) % 2
            start = offsets[h][-1]
            away = pl.multiple_of(start + (1 - bit) * size, 16)
            sends[step][:, h * side : (h + 1) * side] = acc[
                pl.ds(away, size), h * side : (h + 1) * side
            ].astype(jnp.bfloat16)
            reduce_copy(step, h, flipped(s, 1 << place)).start()
            offsets[h].append(start + bit * size)
        for h in range(2):
            place = orders[h][step - 1]
            reduce_copy(step, h, flipped(s, 1 << place)).wait_recv()
            keep = pl.ds(pl.multiple_of(offsets[h][-1], 16), size)
            cut = slice(h * side, (h + 1) * side)
            acc[keep, cut] += recvs[step][:, cut].astype(jnp.float32)
    size = rows >> bits
    for h in range(2):
        at = offsets[h][-1]
        cut = slice(h * side, (h + 1) * side)
        wg_ref[pl.ds(pl.multiple_of(low * big + at, 16), size), cut] = acc[
            pl.ds(pl.multiple_of(at, 16), size), cut
        ].astype(jnp.bfloat16)

    def spread_copy(step, h, incoming):
        place = orders[h][step - 1]
        bit = s // (1 << place) % 2
        size = rows >> (step + 1)
        at = low * big + offsets[h][step - 1] + ((1 - bit) if incoming else bit) * size
        block = wg_ref.at[pl.ds(pl.multiple_of(at, 16), size), pl.ds(h * side, side)]
        return pltpu.make_async_remote_copy(
            src_ref=block,
            dst_ref=block,
            send_sem=asend.at[step, h],
            recv_sem=arecv.at[step, h],
            device_id=(flipped(s, 1 << place), z),
            device_id_type=mesh_id,
        )

    for step in range(bits - 1, 0, -1):
        for h in range(2):
            spread_copy(step, h, False).start()
        for h in range(2):
            spread_copy(step, h, True).wait_recv()

    def last_copy(incoming):
        block = wg_ref.at[pl.ds(pl.multiple_of(((1 - low) if incoming else low) * big, 16), big), :]
        return pltpu.make_async_remote_copy(
            src_ref=block,
            dst_ref=block,
            send_sem=asend.at[0, 0],
            recv_sem=arecv.at[0, 0],
            device_id=(sibling, z),
            device_id_type=mesh_id,
        )

    last_copy(False).start()
    last_copy(True).wait_recv()
    for offset in range(1, reach + 1):

        @pl.when(linear >= offset)
        def _():
            halo_copy(offset, False).wait_send()

    for gap in range(1, groups):
        gather_copy(gap, False).wait_send()
    reduce_copy(0, None, sibling).wait_send()
    for step in range(1, bits):
        for h in range(2):
            reduce_copy(step, h, flipped(s, 1 << orders[h][step - 1])).wait_send()
            spread_copy(step, h, False).wait_send()
    last_copy(False).wait_send()


def finish(back, own, weights, columns, reach):
    seqs = lax.axis_size("seq")
    groups = lax.axis_size("fsdp")
    tok, cols = own.shape
    rows = columns.shape[1]
    bits = seqs.bit_length() - 1
    vmem = pl.BlockSpec(memory_space=pltpu.VMEM)
    steps = [pltpu.VMEM((rows >> (k + 1), cols), jnp.bfloat16) for k in range(bits)]
    dma = pltpu.SemaphoreType.DMA
    return pl.pallas_call(
        functools.partial(finish_kernel, seqs, groups, reach),
        out_shape=[
            jax.ShapeDtypeStruct((tok, weights.shape[0]), jnp.bfloat16),
            jax.ShapeDtypeStruct((rows, cols), jnp.bfloat16),
        ],
        in_specs=[vmem] * 4,
        out_specs=[vmem] * 2,
        scratch_shapes=[
            pltpu.VMEM((reach, tok, cols), jnp.bfloat16),
            pltpu.VMEM((groups, tok, cols), jnp.bfloat16),
            pltpu.VMEM((tok, cols), jnp.bfloat16),
            pltpu.VMEM((rows // 2, cols), jnp.float32),
            steps,
            steps,
            dma((reach,)),
            dma((reach,)),
            dma((groups - 1,)),
            dma((groups - 1,)),
            dma((bits, 2)),
            dma((bits, 2)),
            dma((bits, 2)),
            dma((bits, 2)),
        ],
        compiler_params=pltpu.CompilerParams(has_side_effects=True),
        name="finish",
    )(back, own, weights, columns)


def body(hidden, kv_blocks, kv_scale, queries, grad_out):
    tok = hidden.shape[0]
    groups = lax.axis_size("fsdp")
    reach = groups // 2
    weights, kv = project(hidden, kv_blocks, kv_scale)
    pieces = []
    for offset in range(reach, 0, -1):
        pieces.append(shifted(kv, ("seq", "fsdp"), offset))
    window = jnp.concatenate(pieces + [kv], axis=0)
    window, later = lax.optimization_barrier((window, hidden))
    columns = lax.all_to_all(later, "fsdp", split_axis=1, concat_axis=0, tiled=True)
    attn_out, grad_queries, dwin = attend(queries, window, grad_out, reach)
    back = dwin[: reach * tok].astype(jnp.bfloat16)
    own = dwin[reach * tok :]
    grad_hidden, weight_grad = finish(back, own, weights, columns, reach)
    return (attn_out, grad_queries, grad_hidden, weight_grad.astype(jnp.float32))


def solution(mesh):
    return jax.shard_map(
        body,
        mesh=mesh,
        in_specs=(
            P(("seq", "fsdp"), None),
            P("fsdp", None),
            P("fsdp", None),
            P(("seq", "fsdp"), None),
            P(("seq", "fsdp"), None),
        ),
        out_specs=(
            P(("seq", "fsdp"), None),
            P(("seq", "fsdp"), None),
            P(("seq", "fsdp"), None),
            P("fsdp", None),
        ),
        check_vma=False,
    )
```

```python
import functools

import jax
import jax.numpy as jnp
from jax import lax
from jax.experimental import pallas as pl
from jax.experimental.pallas import tpu as pltpu
from jax.sharding import PartitionSpec as P

HEADS = 32
KV_HEADS = 4
HEAD = 128
QB = 128


NEG = -1e30


def shifted(block, axis, distance):
    devices = range(lax.axis_size(axis))
    route = [(i - distance, i) for i in devices if i - distance in devices]
    return lax.ppermute(block, axis, route)


def attend_kernel(reach, q_ref, g_ref, k_ref, v_ref, out_ref, dq_ref, dk_ref, dv_ref):
    tok = q_ref.shape[0]
    group = q_ref.shape[1] // HEAD
    count = k_ref.shape[0]
    span = reach * tok
    factor = 1.0 / float(HEAD) ** 0.5
    base = (lax.axis_index("seq") * lax.axis_size("fsdp") + lax.axis_index("fsdp")) * tok
    row = lax.broadcasted_iota(jnp.int32, (tok, count), 0)
    col = lax.broadcasted_iota(jnp.int32, (tok, count), 1)
    allowed = (col > row) & (col <= row + span) & (col >= span - base)
    keys = k_ref[...]
    values = v_ref[...]
    nt = (((1,), (1,)), ((), ()))
    tn = (((0,), (0,)), ((), ()))
    ps, ds, qs, gs = [], [], [], []
    for h in range(group):
        cut = slice(h * HEAD, (h + 1) * HEAD)
        q = q_ref[:, cut]
        g = g_ref[:, cut]
        scores = lax.dot_general(q, keys, nt, preferred_element_type=jnp.float32) * factor
        scores = jnp.where(allowed, scores, NEG)
        expd = jnp.exp(scores - jnp.max(scores, axis=-1, keepdims=True))
        probs = expd * (1.0 / jnp.sum(expd, axis=-1, keepdims=True))
        probs_b = probs.astype(jnp.bfloat16)
        out_ref[:, cut] = jnp.dot(probs_b, values, preferred_element_type=jnp.float32).astype(jnp.bfloat16)
        dprobs = lax.dot_general(g, values, nt, preferred_element_type=jnp.float32)
        delta = jnp.sum(probs * dprobs, axis=-1, keepdims=True)
        dscores = (probs * (dprobs - delta) * factor).astype(jnp.bfloat16)
        dq_ref[:, cut] = jnp.dot(dscores, keys, preferred_element_type=jnp.float32).astype(jnp.bfloat16)
        ps.append(probs_b)
        ds.append(dscores)
        qs.append(q)
        gs.append(g)
    cat = lambda parts: jnp.concatenate(parts, axis=0)
    dk_ref[...] = lax.dot_general(cat(ds), cat(qs), tn, preferred_element_type=jnp.float32)
    dv_ref[...] = lax.dot_general(cat(ps), cat(gs), tn, preferred_element_type=jnp.float32)


def attend(queries, window, grad_out, reach):
    tok, width = queries.shape
    count = window.shape[0]
    heads = window.shape[1] // (2 * HEAD)
    wide = pl.BlockSpec((tok, width // heads), lambda i: (0, i))
    key = pl.BlockSpec((count, HEAD), lambda i: (0, i))
    value = pl.BlockSpec((count, HEAD), lambda i: (0, i + heads))
    out, dq, dk, dv = pl.pallas_call(
        functools.partial(attend_kernel, reach),
        grid=(heads,),
        in_specs=[wide, wide, key, value],
        out_specs=[wide, wide, key, key],
        out_shape=[
            jax.ShapeDtypeStruct((tok, width), jnp.bfloat16),
            jax.ShapeDtypeStruct((tok, width), jnp.bfloat16),
            jax.ShapeDtypeStruct((count, heads * HEAD), jnp.float32),
            jax.ShapeDtypeStruct((count, heads * HEAD), jnp.float32),
        ],
        cost_estimate=pl.CostEstimate(flops=12 * tok * width * count, bytes_accessed=8 * tok * width, transcendentals=0),
        name="attend",
    )(queries, grad_out, window, window)
    return out, dq, jnp.concatenate([dk, dv], axis=1)


def flipped(index, mask):
    for place in range(mask.bit_length()):
        if mask >> place & 1:
            index = index + (1 << place) * (1 - 2 * (index // (1 << place) % 2))
    return index


def orders_of(bits):
    return (list(range(1, bits)) + [0], list(range(bits - 1, 0, -1)) + [0])


def project_kernel(seqs, groups, hid_ref, blk_ref, sc_ref, w_ref, kv_ref, col_ref, acc, zsend, zrecv, qsend, qrecv, csend, crecv):
    s = lax.axis_index("seq")
    z = lax.axis_index("fsdp")
    rows = blk_ref.shape[0]
    unit = rows // seqs
    half = unit // 2
    bits = seqs.bit_length() - 1
    chunk = min(512, rows)

    def scale_block(i, carry):
        at = pl.multiple_of(i * QB, QB)
        block = blk_ref[pl.ds(at, QB), :].astype(jnp.float32) * sc_ref[pl.ds(i, 1), :]
        w_ref[pl.ds(pl.multiple_of(z * rows + at, QB), QB), :] = block.astype(jnp.bfloat16)
        return carry

    lax.fori_loop(0, rows // QB, scale_block, 0)

    def line_copy(shard, up, h):
        piece = w_ref.at[pl.ds(pl.multiple_of(shard * rows + s * unit + h * half, 16), half), :]
        return pltpu.make_async_remote_copy(
            src_ref=piece,
            dst_ref=piece,
            send_sem=zsend.at[up, shard, h],
            recv_sem=zrecv.at[shard, h],
            device_id=(s, z + 1 if up else z - 1),
            device_id_type=pl.DeviceIdType.MESH,
        )

    def cube_copy(turn, shard, order, step, which, incoming):
        bit = order[step]
        mask = 0
        for k in range(step):
            if which >> k & 1:
                mask |= 1 << order[k]
        h = 0 if order is orders[0] else 1
        owner = flipped(s, mask | (1 << bit) if incoming else mask)
        piece = w_ref.at[pl.ds(pl.multiple_of(shard * rows + owner * unit + h * half, 16), half), :]
        slot = (1 << step) - 1 + which
        return pltpu.make_async_remote_copy(
            src_ref=piece,
            dst_ref=piece,
            send_sem=qsend.at[turn, h, slot],
            recv_sem=qrecv.at[turn, h, slot],
            device_id=(flipped(s, 1 << bit), z),
            device_id_type=pl.DeviceIdType.MESH,
        )

    orders = orders_of(bits)
    near = jnp.minimum(z, groups - 1 - z)

    def shard_at(turn):
        step = turn // 2 + 1
        paired = z - step if turn % 2 == 0 else z + step
        far = turn - near + 1
        single = jnp.where(z > groups - 1 - z, z - far, z + far)
        return jnp.where(turn < 2 * near, paired, single)

    shards = [shard_at(turn) for turn in range(groups - 1)]

    for h in range(2):

        @pl.when(z < groups - 1)
        def _():
            line_copy(z, 1, h).start()

        @pl.when(z > 0)
        def _():
            line_copy(z, 0, h).start()

    def column_copy(gap, incoming):
        other = (z - gap + groups) % groups if incoming else (z + gap) % groups
        part = pl.multiple_of(other * rows, 128)
        return pltpu.make_async_remote_copy(
            src_ref=hid_ref.at[:, pl.ds(part, rows)],
            dst_ref=col_ref.at[other if incoming else z],
            send_sem=csend.at[gap - 1],
            recv_sem=crecv.at[gap - 1],
            device_id=(s, other),
            device_id_type=pl.DeviceIdType.MESH,
        )

    acc[...] = jnp.zeros_like(acc)

    def multiply(shard):
        def part(i, carry):
            at = pl.multiple_of(shard * rows + i * chunk, 128)
            acc[...] += jnp.dot(
                hid_ref[:, pl.ds(at, chunk)], w_ref[pl.ds(at, chunk), :], preferred_element_type=jnp.float32
            )
            return carry

        lax.fori_loop(0, rows // chunk, part, 0)

    multiply(z)
    col_ref[z] = hid_ref[:, pl.ds(pl.multiple_of(z * rows, 128), rows)]
    turns = 2 * (groups - 1)
    for tick in range(turns + bits):
        for stage in range(bits, -1, -1):
            if not 0 <= tick - stage < turns:
                continue
            turn, h = divmod(tick - stage, 2)
            order = orders[h]
            shard = shards[turn]
            if stage == 0:
                line_copy(shard, 0, h).wait_recv()

                @pl.when((shard < z) & (z < groups - 1))
                def _():
                    line_copy(shard, 1, h).start()

                @pl.when((shard > z) & (z > 0))
                def _():
                    line_copy(shard, 0, h).start()
            else:
                for which in range(1 << (stage - 1)):
                    cube_copy(turn, shard, order, stage - 1, which, True).wait_recv()
            if stage < bits:
                for which in range(1 << stage):
                    cube_copy(turn, shard, order, stage, which, False).start()
            elif h == 1:
                multiply(shard)
        if tick == max(turns - 3, 0):
            for gap in range(1, groups):
                column_copy(gap, False).start()
    kv_ref[...] = acc[...].astype(jnp.bfloat16)
    for gap in range(1, groups):
        column_copy(gap, True).wait_recv()
        column_copy(gap, False).wait_send()
    for shard in range(groups):
        for h in range(2):

            @pl.when((shard <= z) & (z < groups - 1))
            def _():
                line_copy(shard, 1, h).wait_send()

            @pl.when((shard >= z) & (z > 0))
            def _():
                line_copy(shard, 0, h).wait_send()

    for turn in range(groups - 1):
        for order in orders:
            for stage in range(bits):
                for which in range(1 << stage):
                    cube_copy(turn, shards[turn], order, stage, which, False).wait_send()


def project(hidden, kv_blocks, kv_scale):
    seqs = lax.axis_size("seq")
    groups = lax.axis_size("fsdp")
    tok, width = hidden.shape
    cols = kv_blocks.shape[1]
    spread = jnp.repeat(kv_scale, QB, axis=1)
    vmem = pl.BlockSpec(memory_space=pltpu.VMEM)
    return pl.pallas_call(
        functools.partial(project_kernel, seqs, groups),
        out_shape=[
            jax.ShapeDtypeStruct((width, cols), jnp.bfloat16),
            jax.ShapeDtypeStruct((tok, cols), jnp.bfloat16),
            jax.ShapeDtypeStruct((groups, tok, kv_blocks.shape[0]), jnp.bfloat16),
        ],
        in_specs=[vmem] * 3,
        out_specs=[vmem] * 3,
        scratch_shapes=[
            pltpu.VMEM((tok, cols), jnp.float32),
            pltpu.SemaphoreType.DMA((2, groups, 2)),
            pltpu.SemaphoreType.DMA((groups, 2)),
            pltpu.SemaphoreType.DMA((groups - 1, 2, seqs - 1)),
            pltpu.SemaphoreType.DMA((groups - 1, 2, seqs - 1)),
            pltpu.SemaphoreType.DMA((groups - 1,)),
            pltpu.SemaphoreType.DMA((groups - 1,)),
        ],
        compiler_params=pltpu.CompilerParams(has_side_effects=True),
        name="project",
    )(hidden, kv_blocks, spread)


def finish_kernel(
    seqs, groups, reach, back_ref, own_ref, w_ref, col_ref, gh_ref, wg_ref,
    ret, every, inside, acc, sends, recvs, hsend, hrecv, gsend, grecv, rsend, rrecv, asend, arecv,
):
    s = lax.axis_index("seq")
    z = lax.axis_index("fsdp")
    linear = s * groups + z
    devices = seqs * groups
    tok, cols = own_ref.shape
    rows = col_ref.shape[1]
    bits = seqs.bit_length() - 1
    mesh_id = pl.DeviceIdType.MESH

    def halo_copy(offset, incoming):
        other = linear + offset if incoming else linear - offset
        return pltpu.make_async_remote_copy(
            src_ref=back_ref.at[pl.ds((reach - offset) * tok, tok), :],
            dst_ref=ret.at[offset - 1],
            send_sem=hsend.at[offset - 1],
            recv_sem=hrecv.at[offset - 1],
            device_id=(other // groups, other % groups),
            device_id_type=mesh_id,
        )

    for offset in range(1, reach + 1):

        @pl.when(linear >= offset)
        def _():
            halo_copy(offset, False).start()

    for offset in range(1, reach + 1):

        @pl.when(linear + offset < devices)
        def _():
            halo_copy(offset, True).wait_recv()

        @pl.when(linear + offset >= devices)
        def _():
            ret[offset - 1] = jnp.zeros((tok, cols), jnp.bfloat16)

    total = own_ref[...]
    seg = total
    for offset in range(1, reach + 1):
        piece = ret[offset - 1].astype(jnp.float32)
        total = total + piece
        seg = seg + piece * jnp.where(z + offset < groups, 1.0, 0.0)
    every[z] = total.astype(jnp.bfloat16)
    inside[...] = seg.astype(jnp.bfloat16)

    def gather_copy(gap, incoming):
        other = (z - gap + groups) % groups if incoming else (z + gap) % groups
        block = every.at[other if incoming else z]
        return pltpu.make_async_remote_copy(
            src_ref=block,
            dst_ref=block,
            send_sem=gsend.at[gap - 1],
            recv_sem=grecv.at[gap - 1],
            device_id=(s, other),
            device_id_type=mesh_id,
        )

    for gap in range(1, groups):
        gather_copy(gap, False).start()

    wide = 512

    def spread(i, carry):
        at = pl.multiple_of(i * wide, wide)
        gh_ref[:, pl.ds(at, wide)] = lax.dot_general(
            inside[...], w_ref[pl.ds(at, wide), :], (((1,), (1,)), ((), ())), preferred_element_type=jnp.float32
        ).astype(jnp.bfloat16)
        return carry

    lax.fori_loop(0, w_ref.shape[0] // wide, spread, 0)
    for gap in range(1, groups):
        gather_copy(gap, True).wait_recv()

    big = rows // 2
    tile = min(256, big)
    low = s % 2
    sibling = flipped(s, 1)
    grads = every[...].reshape(groups * tok, cols)

    def product(at):
        return lax.dot_general(
            col_ref[:, pl.ds(at, tile)], grads, (((0,), (0,)), ((), ())), preferred_element_type=jnp.float32
        )

    def theirs(i, carry):
        at = pl.multiple_of(i * tile, tile)
        sends[0][pl.ds(at, tile), :] = product(pl.multiple_of((1 - low) * big + at, tile)).astype(jnp.bfloat16)
        return carry

    lax.fori_loop(0, big // tile, theirs, 0)

    def reduce_copy(step, h, peer):
        cut = slice(None) if h is None else pl.ds(h * (cols // 2), cols // 2)
        return pltpu.make_async_remote_copy(
            src_ref=sends[step].at[:, cut] if h is not None else sends[step],
            dst_ref=recvs[step].at[:, cut] if h is not None else recvs[step],
            send_sem=rsend.at[step, h or 0],
            recv_sem=rrecv.at[step, h or 0],
            device_id=(peer, z),
            device_id_type=mesh_id,
        )

    reduce_copy(0, None, sibling).start()

    def mine(i, carry):
        at = pl.multiple_of(i * tile, tile)
        acc[pl.ds(at, tile), :] = product(pl.multiple_of(low * big + at, tile))
        return carry

    lax.fori_loop(0, big // tile, mine, 0)
    reduce_copy(0, None, sibling).wait_recv()

    def fold(i, carry):
        at = pl.multiple_of(i * tile, tile)
        acc[pl.ds(at, tile), :] += recvs[0][pl.ds(at, tile), :].astype(jnp.float32)
        return carry

    lax.fori_loop(0, big // tile, fold, 0)
    orders = (list(range(1, bits)), list(range(bits - 1, 0, -1)))
    offsets = [[0], [0]]
    side = cols // 2
    for step in range(1, bits):
        size = rows >> (step + 1)
        for h in range(2):
            place = orders[h][step - 1]
            bit = s // (1 << place) % 2
            start = offsets[h][-1]
            away = pl.multiple_of(start + (1 - bit) * size, 16)
            sends[step][:, h * side : (h + 1) * side] = acc[
                pl.ds(away, size), h * side : (h + 1) * side
            ].astype(jnp.bfloat16)
            reduce_copy(step, h, flipped(s, 1 << place)).start()
            offsets[h].append(start + bit * size)
        for h in range(2):
            place = orders[h][step - 1]
            reduce_copy(step, h, flipped(s, 1 << place)).wait_recv()
            keep = pl.ds(pl.multiple_of(offsets[h][-1], 16), size)
            cut = slice(h * side, (h + 1) * side)
            acc[keep, cut] += recvs[step][:, cut].astype(jnp.float32)
    size = rows >> bits
    for h in range(2):
        at = offsets[h][-1]
        cut = slice(h * side, (h + 1) * side)
        wg_ref[pl.ds(pl.multiple_of(low * big + at, 16), size), cut] = acc[
            pl.ds(pl.multiple_of(at, 16), size), cut
        ].astype(jnp.bfloat16)

    def spread_copy(step, h, incoming):
        place = orders[h][step - 1]
        bit = s // (1 << place) % 2
        size = rows >> (step + 1)
        at = low * big + offsets[h][step - 1] + ((1 - bit) if incoming else bit) * size
        block = wg_ref.at[pl.ds(pl.multiple_of(at, 16), size), pl.ds(h * side, side)]
        return pltpu.make_async_remote_copy(
            src_ref=block,
            dst_ref=block,
            send_sem=asend.at[step, h],
            recv_sem=arecv.at[step, h],
            device_id=(flipped(s, 1 << place), z),
            device_id_type=mesh_id,
        )

    for step in range(bits - 1, 0, -1):
        for h in range(2):
            spread_copy(step, h, False).start()
        for h in range(2):
            spread_copy(step, h, True).wait_recv()

    def last_copy(incoming):
        block = wg_ref.at[pl.ds(pl.multiple_of(((1 - low) if incoming else low) * big, 16), big), :]
        return pltpu.make_async_remote_copy(
            src_ref=block,
            dst_ref=block,
            send_sem=asend.at[0, 0],
            recv_sem=arecv.at[0, 0],
            device_id=(sibling, z),
            device_id_type=mesh_id,
        )

    last_copy(False).start()
    last_copy(True).wait_recv()
    for offset in range(1, reach + 1):

        @pl.when(linear >= offset)
        def _():
            halo_copy(offset, False).wait_send()

    for gap in range(1, groups):
        gather_copy(gap, False).wait_send()
    reduce_copy(0, None, sibling).wait_send()
    for step in range(1, bits):
        for h in range(2):
            reduce_copy(step, h, flipped(s, 1 << orders[h][step - 1])).wait_send()
            spread_copy(step, h, False).wait_send()
    last_copy(False).wait_send()


def finish(back, own, weights, columns, reach):
    seqs = lax.axis_size("seq")
    groups = lax.axis_size("fsdp")
    tok, cols = own.shape
    rows = columns.shape[1]
    bits = seqs.bit_length() - 1
    vmem = pl.BlockSpec(memory_space=pltpu.VMEM)
    steps = [pltpu.VMEM((rows >> (k + 1), cols), jnp.bfloat16) for k in range(bits)]
    dma = pltpu.SemaphoreType.DMA
    return pl.pallas_call(
        functools.partial(finish_kernel, seqs, groups, reach),
        out_shape=[
            jax.ShapeDtypeStruct((tok, weights.shape[0]), jnp.bfloat16),
            jax.ShapeDtypeStruct((rows, cols), jnp.bfloat16),
        ],
        in_specs=[vmem] * 4,
        out_specs=[vmem] * 2,
        scratch_shapes=[
            pltpu.VMEM((reach, tok, cols), jnp.bfloat16),
            pltpu.VMEM((groups, tok, cols), jnp.bfloat16),
            pltpu.VMEM((tok, cols), jnp.bfloat16),
            pltpu.VMEM((rows // 2, cols), jnp.float32),
            steps,
            steps,
            dma((reach,)),
            dma((reach,)),
            dma((groups - 1,)),
            dma((groups - 1,)),
            dma((bits, 2)),
            dma((bits, 2)),
            dma((bits, 2)),
            dma((bits, 2)),
        ],
        compiler_params=pltpu.CompilerParams(has_side_effects=True),
        name="finish",
    )(back, own, weights, columns)


def body(hidden, kv_blocks, kv_scale, queries, grad_out):
    tok = hidden.shape[0]
    groups = lax.axis_size("fsdp")
    reach = groups // 2
    weights, kv, columns = project(hidden, kv_blocks, kv_scale)
    pieces = []
    for offset in range(reach, 0, -1):
        pieces.append(shifted(kv, ("seq", "fsdp"), offset))
    window = jnp.concatenate(pieces + [kv], axis=0)
    columns = columns.reshape(groups * tok, columns.shape[2])
    attn_out, grad_queries, dwin = attend(queries, window, grad_out, reach)
    back = dwin[: reach * tok].astype(jnp.bfloat16)
    own = dwin[reach * tok :]
    grad_hidden, weight_grad = finish(back, own, weights, columns, reach)
    return (attn_out, grad_queries, grad_hidden, weight_grad.astype(jnp.float32))


def solution(mesh):
    return jax.shard_map(
        body,
        mesh=mesh,
        in_specs=(
            P(("seq", "fsdp"), None),
            P("fsdp", None),
            P("fsdp", None),
            P(("seq", "fsdp"), None),
            P(("seq", "fsdp"), None),
        ),
        out_specs=(
            P(("seq", "fsdp"), None),
            P(("seq", "fsdp"), None),
            P(("seq", "fsdp"), None),
            P("fsdp", None),
        ),
        check_vma=False,
    )
```

```python
import functools

import jax
import jax.numpy as jnp
from jax import lax
from jax.experimental import pallas as pl
from jax.experimental.pallas import tpu as pltpu
from jax.sharding import PartitionSpec as P

HEADS = 32
KV_HEADS = 4
HEAD = 128
QB = 128


NEG = -1e30


def shifted(block, axis, distance):
    devices = range(lax.axis_size(axis))
    route = [(i - distance, i) for i in devices if i - distance in devices]
    return lax.ppermute(block, axis, route)


def attend_kernel(reach, q_ref, g_ref, k_ref, v_ref, out_ref, dq_ref, dk_ref, dv_ref):
    tok = q_ref.shape[0]
    group = q_ref.shape[1] // HEAD
    count = k_ref.shape[0]
    span = reach * tok
    factor = 1.0 / float(HEAD) ** 0.5
    base = (lax.axis_index("seq") * lax.axis_size("fsdp") + lax.axis_index("fsdp")) * tok
    row = lax.broadcasted_iota(jnp.int32, (tok, count), 0)
    col = lax.broadcasted_iota(jnp.int32, (tok, count), 1)
    allowed = (col > row) & (col <= row + span) & (col >= span - base)
    keys = k_ref[...]
    values = v_ref[...]
    nt = (((1,), (1,)), ((), ()))
    tn = (((0,), (0,)), ((), ()))
    ps, ds, qs, gs = [], [], [], []
    for h in range(group):
        cut = slice(h * HEAD, (h + 1) * HEAD)
        q = q_ref[:, cut]
        g = g_ref[:, cut]
        scores = lax.dot_general(q, keys, nt, preferred_element_type=jnp.float32) * factor
        scores = jnp.where(allowed, scores, NEG)
        expd = jnp.exp(scores - jnp.max(scores, axis=-1, keepdims=True))
        probs = expd * (1.0 / jnp.sum(expd, axis=-1, keepdims=True))
        probs_b = probs.astype(jnp.bfloat16)
        out_ref[:, cut] = jnp.dot(probs_b, values, preferred_element_type=jnp.float32).astype(jnp.bfloat16)
        dprobs = lax.dot_general(g, values, nt, preferred_element_type=jnp.float32)
        delta = jnp.sum(probs * dprobs, axis=-1, keepdims=True)
        dscores = (probs * (dprobs - delta) * factor).astype(jnp.bfloat16)
        dq_ref[:, cut] = jnp.dot(dscores, keys, preferred_element_type=jnp.float32).astype(jnp.bfloat16)
        ps.append(probs_b)
        ds.append(dscores)
        qs.append(q)
        gs.append(g)
    cat = lambda parts: jnp.concatenate(parts, axis=0)
    dk_ref[...] = lax.dot_general(cat(ds), cat(qs), tn, preferred_element_type=jnp.float32)
    dv_ref[...] = lax.dot_general(cat(ps), cat(gs), tn, preferred_element_type=jnp.float32)


def attend(queries, window, grad_out, reach):
    tok, width = queries.shape
    count = window.shape[0]
    heads = window.shape[1] // (2 * HEAD)
    wide = pl.BlockSpec((tok, width // heads), lambda i: (0, i))
    key = pl.BlockSpec((count, HEAD), lambda i: (0, i))
    value = pl.BlockSpec((count, HEAD), lambda i: (0, i + heads))
    out, dq, dk, dv = pl.pallas_call(
        functools.partial(attend_kernel, reach),
        grid=(heads,),
        in_specs=[wide, wide, key, value],
        out_specs=[wide, wide, key, key],
        out_shape=[
            jax.ShapeDtypeStruct((tok, width), jnp.bfloat16),
            jax.ShapeDtypeStruct((tok, width), jnp.bfloat16),
            jax.ShapeDtypeStruct((count, heads * HEAD), jnp.float32),
            jax.ShapeDtypeStruct((count, heads * HEAD), jnp.float32),
        ],
        cost_estimate=pl.CostEstimate(flops=12 * tok * width * count, bytes_accessed=8 * tok * width, transcendentals=0),
        name="attend",
    )(queries, grad_out, window, window)
    return out, dq, jnp.concatenate([dk, dv], axis=1)


def flipped(index, mask):
    for place in range(mask.bit_length()):
        if mask >> place & 1:
            index = index + (1 << place) * (1 - 2 * (index // (1 << place) % 2))
    return index


def orders_of(bits):
    return (list(range(1, bits)) + [0], list(range(bits - 1, 0, -1)) + [0])


def project_kernel(seqs, groups, hid_ref, blk_ref, sc_ref, out_ref, kv_ref, col_ref, w_ref, acc, zsend, zrecv, qsend, qrecv, csend, crecv, wsem):
    s = lax.axis_index("seq")
    z = lax.axis_index("fsdp")
    rows = blk_ref.shape[0]
    unit = rows // seqs
    half = unit // 2
    bits = seqs.bit_length() - 1
    chunk = min(512, rows)

    def scale_block(i, carry):
        at = pl.multiple_of(i * QB, QB)
        block = blk_ref[pl.ds(at, QB), :].astype(jnp.float32) * sc_ref[pl.ds(i, 1), :]
        w_ref[pl.ds(pl.multiple_of(z * rows + at, QB), QB), :] = block.astype(jnp.bfloat16)
        return carry

    lax.fori_loop(0, rows // QB, scale_block, 0)

    def line_copy(shard, up):
        piece = w_ref.at[pl.ds(pl.multiple_of(shard * rows + s * unit, 16), unit), :]
        return pltpu.make_async_remote_copy(
            src_ref=piece,
            dst_ref=piece,
            send_sem=zsend.at[up, shard],
            recv_sem=zrecv.at[shard],
            device_id=(s, z + 1 if up else z - 1),
            device_id_type=pl.DeviceIdType.MESH,
        )

    def cube_copy(turn, shard, order, step, which, incoming):
        bit = order[step]
        mask = 0
        for k in range(step):
            if which >> k & 1:
                mask |= 1 << order[k]
        h = 0 if order is orders[0] else 1
        owner = flipped(s, mask | (1 << bit) if incoming else mask)
        piece = w_ref.at[pl.ds(pl.multiple_of(shard * rows + owner * unit + h * half, 16), half), :]
        slot = (1 << step) - 1 + which
        return pltpu.make_async_remote_copy(
            src_ref=piece,
            dst_ref=piece,
            send_sem=qsend.at[turn, h, slot],
            recv_sem=qrecv.at[turn, h, slot],
            device_id=(flipped(s, 1 << bit), z),
            device_id_type=pl.DeviceIdType.MESH,
        )

    orders = orders_of(bits)
    near = jnp.minimum(z, groups - 1 - z)

    def shard_at(turn):
        step = turn // 2 + 1
        paired = z - step if turn % 2 == 0 else z + step
        far = turn - near + 1
        single = jnp.where(z > groups - 1 - z, z - far, z + far)
        return jnp.where(turn < 2 * near, paired, single)

    shards = [shard_at(turn) for turn in range(groups - 1)]

    @pl.when(z < groups - 1)
    def _():
        line_copy(z, 1).start()

    @pl.when(z > 0)
    def _():
        line_copy(z, 0).start()

    def column_copy(gap, incoming):
        other = (z - gap + groups) % groups if incoming else (z + gap) % groups
        part = pl.multiple_of(other * rows, 128)
        return pltpu.make_async_remote_copy(
            src_ref=hid_ref.at[:, pl.ds(part, rows)],
            dst_ref=col_ref.at[other if incoming else z],
            send_sem=csend.at[gap - 1],
            recv_sem=crecv.at[gap - 1],
            device_id=(s, other),
            device_id_type=pl.DeviceIdType.MESH,
        )

    acc[...] = jnp.zeros_like(acc)

    def store_copy(turn, shard):
        part = pl.ds(pl.multiple_of(shard * rows, 16), rows)
        return pltpu.make_async_copy(w_ref.at[part, :], out_ref.at[part, :], wsem.at[turn])

    def multiply(shard):
        def part(i, carry):
            at = pl.multiple_of(shard * rows + i * chunk, 128)
            acc[...] += jnp.dot(
                hid_ref[:, pl.ds(at, chunk)], w_ref[pl.ds(at, chunk), :], preferred_element_type=jnp.float32
            )
            return carry

        lax.fori_loop(0, rows // chunk, part, 0)

    multiply(z)
    store_copy(groups - 1, z).start()
    col_ref[z] = hid_ref[:, pl.ds(pl.multiple_of(z * rows, 128), rows)]
    for tick in range(groups - 1 + bits):
        for stage in range(bits, -1, -1):
            turn = tick - stage
            if turn < 0 or turn >= groups - 1:
                continue
            shard = shards[turn]
            if stage == 0:
                line_copy(shard, 0).wait_recv()

                @pl.when((shard < z) & (z < groups - 1))
                def _():
                    line_copy(shard, 1).start()

                @pl.when((shard > z) & (z > 0))
                def _():
                    line_copy(shard, 0).start()
            else:
                for order in orders:
                    for which in range(1 << (stage - 1)):
                        cube_copy(turn, shard, order, stage - 1, which, True).wait_recv()
            if stage < bits:
                for order in orders:
                    for which in range(1 << stage):
                        cube_copy(turn, shard, order, stage, which, False).start()
            else:
                multiply(shard)
                store_copy(turn, shard).start()
        if tick == groups - 2:
            for gap in range(1, groups):
                column_copy(gap, False).start()
    kv_ref[...] = acc[...].astype(jnp.bfloat16)
    for turn in range(groups - 1):
        store_copy(turn, shards[turn]).wait()
    store_copy(groups - 1, z).wait()
    for gap in range(1, groups):
        column_copy(gap, True).wait_recv()
        column_copy(gap, False).wait_send()
    for shard in range(groups):

        @pl.when((shard <= z) & (z < groups - 1))
        def _():
            line_copy(shard, 1).wait_send()

        @pl.when((shard >= z) & (z > 0))
        def _():
            line_copy(shard, 0).wait_send()

    for turn in range(groups - 1):
        for order in orders:
            for stage in range(bits):
                for which in range(1 << stage):
                    cube_copy(turn, shards[turn], order, stage, which, False).wait_send()


def project(hidden, kv_blocks, kv_scale):
    seqs = lax.axis_size("seq")
    groups = lax.axis_size("fsdp")
    tok, width = hidden.shape
    cols = kv_blocks.shape[1]
    spread = jnp.repeat(kv_scale, QB, axis=1)
    vmem = pl.BlockSpec(memory_space=pltpu.VMEM)
    return pl.pallas_call(
        functools.partial(project_kernel, seqs, groups),
        out_shape=[
            jax.ShapeDtypeStruct((width, cols), jnp.bfloat16),
            jax.ShapeDtypeStruct((tok, cols), jnp.bfloat16),
            jax.ShapeDtypeStruct((groups, tok, kv_blocks.shape[0]), jnp.bfloat16),
        ],
        in_specs=[vmem] * 3,
        out_specs=[pl.BlockSpec(memory_space=pl.ANY), vmem, vmem],
        scratch_shapes=[
            pltpu.VMEM((width, cols), jnp.bfloat16),
            pltpu.VMEM((tok, cols), jnp.float32),
            pltpu.SemaphoreType.DMA((2, groups)),
            pltpu.SemaphoreType.DMA((groups,)),
            pltpu.SemaphoreType.DMA((groups - 1, 2, seqs - 1)),
            pltpu.SemaphoreType.DMA((groups - 1, 2, seqs - 1)),
            pltpu.SemaphoreType.DMA((groups - 1,)),
            pltpu.SemaphoreType.DMA((groups - 1,)),
            pltpu.SemaphoreType.DMA((groups,)),
        ],
        compiler_params=pltpu.CompilerParams(has_side_effects=True),
        name="project",
    )(hidden, kv_blocks, spread)


def finish_kernel(
    seqs, groups, reach, back_ref, own_ref, in_ref, col_ref, gh_ref, wg_ref,
    w_ref, wsem, ret, every, inside, acc, sends, recvs, hsend, hrecv, gsend, grecv, rsend, rrecv, asend, arecv,
):
    s = lax.axis_index("seq")
    z = lax.axis_index("fsdp")
    linear = s * groups + z
    devices = seqs * groups
    tok, cols = own_ref.shape
    rows = col_ref.shape[1]
    bits = seqs.bit_length() - 1
    mesh_id = pl.DeviceIdType.MESH
    load = pltpu.make_async_copy(in_ref, w_ref, wsem)
    load.start()

    def halo_copy(offset, incoming):
        other = linear + offset if incoming else linear - offset
        return pltpu.make_async_remote_copy(
            src_ref=back_ref.at[pl.ds((reach - offset) * tok, tok), :],
            dst_ref=ret.at[offset - 1],
            send_sem=hsend.at[offset - 1],
            recv_sem=hrecv.at[offset - 1],
            device_id=(other // groups, other % groups),
            device_id_type=mesh_id,
        )

    for offset in range(1, reach + 1):

        @pl.when(linear >= offset)
        def _():
            halo_copy(offset, False).start()

    for offset in range(1, reach + 1):

        @pl.when(linear + offset < devices)
        def _():
            halo_copy(offset, True).wait_recv()

        @pl.when(linear + offset >= devices)
        def _():
            ret[offset - 1] = jnp.zeros((tok, cols), jnp.bfloat16)

    total = own_ref[...]
    seg = total
    for offset in range(1, reach + 1):
        piece = ret[offset - 1].astype(jnp.float32)
        total = total + piece
        seg = seg + piece * jnp.where(z + offset < groups, 1.0, 0.0)
    every[z] = total.astype(jnp.bfloat16)
    inside[...] = seg.astype(jnp.bfloat16)

    def gather_copy(gap, incoming):
        other = (z - gap + groups) % groups if incoming else (z + gap) % groups
        block = every.at[other if incoming else z]
        return pltpu.make_async_remote_copy(
            src_ref=block,
            dst_ref=block,
            send_sem=gsend.at[gap - 1],
            recv_sem=grecv.at[gap - 1],
            device_id=(s, other),
            device_id_type=mesh_id,
        )

    for gap in range(1, groups):
        gather_copy(gap, False).start()

    load.wait()
    wide = 512

    def spread(i, carry):
        at = pl.multiple_of(i * wide, wide)
        gh_ref[:, pl.ds(at, wide)] = lax.dot_general(
            inside[...], w_ref[pl.ds(at, wide), :], (((1,), (1,)), ((), ())), preferred_element_type=jnp.float32
        ).astype(jnp.bfloat16)
        return carry

    lax.fori_loop(0, w_ref.shape[0] // wide, spread, 0)
    for gap in range(1, groups):
        gather_copy(gap, True).wait_recv()

    big = rows // 2
    tile = min(256, big)
    low = s % 2
    sibling = flipped(s, 1)
    grads = every[...].reshape(groups * tok, cols)

    def product(at):
        return lax.dot_general(
            col_ref[:, pl.ds(at, tile)], grads, (((0,), (0,)), ((), ())), preferred_element_type=jnp.float32
        )

    def theirs(i, carry):
        at = pl.multiple_of(i * tile, tile)
        sends[0][pl.ds(at, tile), :] = product(pl.multiple_of((1 - low) * big + at, tile)).astype(jnp.bfloat16)
        return carry

    lax.fori_loop(0, big // tile, theirs, 0)

    def reduce_copy(step, h, peer):
        cut = slice(None) if h is None else pl.ds(h * (cols // 2), cols // 2)
        return pltpu.make_async_remote_copy(
            src_ref=sends[step].at[:, cut] if h is not None else sends[step],
            dst_ref=recvs[step].at[:, cut] if h is not None else recvs[step],
            send_sem=rsend.at[step, h or 0],
            recv_sem=rrecv.at[step, h or 0],
            device_id=(peer, z),
            device_id_type=mesh_id,
        )

    reduce_copy(0, None, sibling).start()

    def mine(i, carry):
        at = pl.multiple_of(i * tile, tile)
        acc[pl.ds(at, tile), :] = product(pl.multiple_of(low * big + at, tile))
        return carry

    lax.fori_loop(0, big // tile, mine, 0)
    reduce_copy(0, None, sibling).wait_recv()

    def fold(i, carry):
        at = pl.multiple_of(i * tile, tile)
        acc[pl.ds(at, tile), :] += recvs[0][pl.ds(at, tile), :].astype(jnp.float32)
        return carry

    lax.fori_loop(0, big // tile, fold, 0)
    orders = (list(range(1, bits)), list(range(bits - 1, 0, -1)))
    offsets = [[0], [0]]
    side = cols // 2
    for step in range(1, bits):
        size = rows >> (step + 1)
        for h in range(2):
            place = orders[h][step - 1]
            bit = s // (1 << place) % 2
            start = offsets[h][-1]
            away = pl.multiple_of(start + (1 - bit) * size, 16)
            sends[step][:, h * side : (h + 1) * side] = acc[
                pl.ds(away, size), h * side : (h + 1) * side
            ].astype(jnp.bfloat16)
            reduce_copy(step, h, flipped(s, 1 << place)).start()
            offsets[h].append(start + bit * size)
        for h in range(2):
            place = orders[h][step - 1]
            reduce_copy(step, h, flipped(s, 1 << place)).wait_recv()
            keep = pl.ds(pl.multiple_of(offsets[h][-1], 16), size)
            cut = slice(h * side, (h + 1) * side)
            acc[keep, cut] += recvs[step][:, cut].astype(jnp.float32)
    size = rows >> bits
    for h in range(2):
        at = offsets[h][-1]
        cut = slice(h * side, (h + 1) * side)
        wg_ref[pl.ds(pl.multiple_of(low * big + at, 16), size), cut] = acc[
            pl.ds(pl.multiple_of(at, 16), size), cut
        ].astype(jnp.bfloat16)

    def spread_copy(step, h, incoming):
        place = orders[h][step - 1]
        bit = s // (1 << place) % 2
        size = rows >> (step + 1)
        at = low * big + offsets[h][step - 1] + ((1 - bit) if incoming else bit) * size
        block = wg_ref.at[pl.ds(pl.multiple_of(at, 16), size), pl.ds(h * side, side)]
        return pltpu.make_async_remote_copy(
            src_ref=block,
            dst_ref=block,
            send_sem=asend.at[step, h],
            recv_sem=arecv.at[step, h],
            device_id=(flipped(s, 1 << place), z),
            device_id_type=mesh_id,
        )

    for step in range(bits - 1, 0, -1):
        for h in range(2):
            spread_copy(step, h, False).start()
        for h in range(2):
            spread_copy(step, h, True).wait_recv()

    def last_copy(incoming):
        block = wg_ref.at[pl.ds(pl.multiple_of(((1 - low) if incoming else low) * big, 16), big), :]
        return pltpu.make_async_remote_copy(
            src_ref=block,
            dst_ref=block,
            send_sem=asend.at[0, 0],
            recv_sem=arecv.at[0, 0],
            device_id=(sibling, z),
            device_id_type=mesh_id,
        )

    last_copy(False).start()
    last_copy(True).wait_recv()
    for offset in range(1, reach + 1):

        @pl.when(linear >= offset)
        def _():
            halo_copy(offset, False).wait_send()

    for gap in range(1, groups):
        gather_copy(gap, False).wait_send()
    reduce_copy(0, None, sibling).wait_send()
    for step in range(1, bits):
        for h in range(2):
            reduce_copy(step, h, flipped(s, 1 << orders[h][step - 1])).wait_send()
            spread_copy(step, h, False).wait_send()
    last_copy(False).wait_send()


def finish(back, own, weights, columns, reach):
    seqs = lax.axis_size("seq")
    groups = lax.axis_size("fsdp")
    tok, cols = own.shape
    rows = columns.shape[1]
    bits = seqs.bit_length() - 1
    vmem = pl.BlockSpec(memory_space=pltpu.VMEM)
    steps = [pltpu.VMEM((rows >> (k + 1), cols), jnp.bfloat16) for k in range(bits)]
    dma = pltpu.SemaphoreType.DMA
    return pl.pallas_call(
        functools.partial(finish_kernel, seqs, groups, reach),
        out_shape=[
            jax.ShapeDtypeStruct((tok, weights.shape[0]), jnp.bfloat16),
            jax.ShapeDtypeStruct((rows, cols), jnp.bfloat16),
        ],
        in_specs=[vmem, vmem, pl.BlockSpec(memory_space=pl.ANY), vmem],
        out_specs=[vmem] * 2,
        scratch_shapes=[
            pltpu.VMEM(weights.shape, jnp.bfloat16),
            dma(()),
            pltpu.VMEM((reach, tok, cols), jnp.bfloat16),
            pltpu.VMEM((groups, tok, cols), jnp.bfloat16),
            pltpu.VMEM((tok, cols), jnp.bfloat16),
            pltpu.VMEM((rows // 2, cols), jnp.float32),
            steps,
            steps,
            dma((reach,)),
            dma((reach,)),
            dma((groups - 1,)),
            dma((groups - 1,)),
            dma((bits, 2)),
            dma((bits, 2)),
            dma((bits, 2)),
            dma((bits, 2)),
        ],
        compiler_params=pltpu.CompilerParams(has_side_effects=True),
        name="finish",
    )(back, own, weights, columns)


def body(hidden, kv_blocks, kv_scale, queries, grad_out):
    tok = hidden.shape[0]
    groups = lax.axis_size("fsdp")
    reach = groups // 2
    weights, kv, columns = project(hidden, kv_blocks, kv_scale)
    pieces = []
    for offset in range(reach, 0, -1):
        pieces.append(shifted(kv, ("seq", "fsdp"), offset))
    window = jnp.concatenate(pieces + [kv], axis=0)
    columns = columns.reshape(groups * tok, columns.shape[2])
    attn_out, grad_queries, dwin = attend(queries, window, grad_out, reach)
    back = dwin[: reach * tok].astype(jnp.bfloat16)
    own = dwin[reach * tok :]
    grad_hidden, weight_grad = finish(back, own, weights, columns, reach)
    return (attn_out, grad_queries, grad_hidden, weight_grad.astype(jnp.float32))


def solution(mesh):
    return jax.shard_map(
        body,
        mesh=mesh,
        in_specs=(
            P(("seq", "fsdp"), None),
            P("fsdp", None),
            P("fsdp", None),
            P(("seq", "fsdp"), None),
            P(("seq", "fsdp"), None),
        ),
        out_specs=(
            P(("seq", "fsdp"), None),
            P(("seq", "fsdp"), None),
            P(("seq", "fsdp"), None),
            P("fsdp", None),
        ),
        check_vma=False,
    )
```
